32 devices in a mesh: prob: 4 (over y, z), feat: 8 (over x, core).
Axes of the slice: x: 4, y: 2, z: 2, core: 2. Of those that a mesh axis runs over, the one named last changes fastest.
The devices are a block of a 4x4x8 slice.
Arguments:
- design: bfloat16 [16384, 4096], P(None, ('prob', 'feat')), parts along dimension 1
- w_init: float32 [4096, 8], P(('prob', 'feat')), parts along dimension 0
- targets: float32 [65536, 8], P('prob'), parts along dimension 0
Outputs:
- output 1: float32 [4096, 8], P(('prob', 'feat')), parts along dimension 0
- output 2: float32 [65536, 8], P('prob'), parts along dimension 0
There are 4 independent parts. The reference program is written for one: setup_inputs(seed, part) draws one part's arguments, and reference() takes and returns one part's arrays. A program takes and returns all parts, laid end to end along the dimension named above; each array names one.
All inputs are finite; a program needn't handle non-finite values.
Results may differ from the reference program's by a relative error of at most 0.00410973.
Values are sent between devices in bfloat16 or wider.
A program may use at most 768 MiB of HBM per device.

```python
import math
import jax
import jax.numpy as jnp
from jax import lax

SAMPLES = 16384
TARGETS = 8
FEAT_DEV = 128
SWEEPS = 6
GROUP = 8
LATENT = 8
LOCAL_STEPS = 2
FEATURES = FEAT_DEV * GROUP
RIDGE = 0.01
GAMMA = 0.75


def latent_scales():
    ratios = 0.6 ** jnp.arange(LATENT, dtype=jnp.float32)
    return ratios * jnp.sqrt(0.5 / jnp.sum(ratios * ratios))


def setup_inputs(seed: int = 0, part: int = 0) -> dict:
    base_key = jax.random.fold_in(jax.random.key(seed), part)
    key_z, key_a, key_e, key_c, key_y, key_w = jax.random.split(base_key, 6)
    scales = latent_scales()
    latent = jax.random.normal(key_z, (SAMPLES, LATENT), jnp.float32)
    loadings = jax.random.normal(key_a, (LATENT, FEATURES), jnp.float32)
    noise = jax.random.normal(key_e, (SAMPLES, FEATURES), jnp.float32)
    design = (jnp.dot(latent * scales, loadings) + math.sqrt(0.5) * noise).astype(jnp.bfloat16)
    coupling = jax.random.normal(key_c, (LATENT, TARGETS), jnp.float32)
    lat_norm = LATENT ** -0.5
    target_noise = jax.random.normal(key_y, (SAMPLES, TARGETS), jnp.float32)
    targets = jnp.dot(latent, coupling) * lat_norm + 0.5 * target_noise
    w_init = jax.random.normal(key_w, (FEATURES, TARGETS), jnp.float32) * (FEATURES ** -0.5)
    return {'design': design, 'w_init': w_init, 'targets': targets}


def block_product(x_block, coef_block):
    full = jnp.dot(x_block, coef_block.astype(jnp.bfloat16), preferred_element_type=jnp.float32)
    return full.astype(jnp.bfloat16).astype(jnp.float32)


def left_product(x_block, resid_part):
    return jnp.dot(x_block.T, resid_part.astype(jnp.bfloat16), preferred_element_type=jnp.float32) / SAMPLES


def block_step(x_block):
    squares = jnp.square(x_block.astype(jnp.float32))
    return SAMPLES / (GROUP * jnp.sum(squares))


def local_passes(x_block, w_block, residual):
    step_size = block_step(x_block)
    gradient = left_product(x_block, residual)
    coef_step = step_size * (gradient - RIDGE * w_block)
    update = block_product(x_block, coef_step)
    for step_idx in range(1, LOCAL_STEPS):
        gradient = left_product(x_block, residual - GROUP * update)
        coef_step = coef_step + step_size * (gradient - RIDGE * (w_block + coef_step))
        update = block_product(x_block, coef_step)
    return coef_step, update


def reference(design, w_init, targets):
    zero_rows = jnp.zeros((SAMPLES, TARGETS), jnp.float32)

    def init_body(total, index):
        x_block = lax.dynamic_slice_in_dim(design, index * FEAT_DEV, FEAT_DEV, axis=1)
        w_block = lax.dynamic_slice_in_dim(w_init, index * FEAT_DEV, FEAT_DEV, axis=0)
        return total + block_product(x_block, w_block), None

    prediction, _ = lax.scan(init_body, zero_rows, jnp.arange(GROUP))

    def sweep_body(carry, unused):
        weights, residual = carry

        def block_body(total, index):
            x_block = lax.dynamic_slice_in_dim(design, index * FEAT_DEV, FEAT_DEV, axis=1)
            w_block = lax.dynamic_slice_in_dim(weights, index * FEAT_DEV, FEAT_DEV, axis=0)
            coef_step, update = local_passes(x_block, w_block, residual)
            return total + update, coef_step

        summed, steps_all = lax.scan(block_body, zero_rows, jnp.arange(GROUP))
        weights = weights + GAMMA * steps_all.reshape(FEATURES, TARGETS)
        residual = residual - GAMMA * summed
        return (weights, residual), None

    (weights, residual), _ = lax.scan(sweep_body, (w_init, targets - prediction), None, length=SWEEPS)
    return weights, residual
```

```python
import functools

import jax
import jax.numpy as jnp
from jax import lax
from jax.experimental import pallas as pl
from jax.experimental.pallas import tpu as pltpu
from jax.sharding import PartitionSpec as P

LOCAL_STEPS = 2
SWEEPS = 6
RIDGE = 0.01
GAMMA = 0.75

LANES = 512
MESH = pl.DeviceIdType.MESH


def kernel(group, chunks, x_hbm, w_ref, y_ref, w_out, r_out,
           x, xt, res, upd, inbox,
           x_sem, y_sem, o_sem, rs_send, rs_recv, ag_send, ag_recv, fw_send):
    chips = group // 2
    width = LANES
    blocks = group * chunks
    samples = x.shape[0]
    me = lax.axis_index("feat")
    chip, core = me // 2, me % 2

    def peer(rel):
        return ((chip + rel // 2) % chips) * 2 + (core + rel % 2) % 2

    def back(rel):
        return ((chips - rel // 2) % chips) * 2 + rel % 2

    near = [2 * d for d in range(1, chips)]
    near.sort(key=lambda rel: min(rel // 2, chips - rel // 2))
    far_first = near[::-1]
    sends = [rel + k for rel in far_first for k in (0, 1)] + [1]
    direct = [1] + near

    def x_copy(b):
        rows = pl.ds(b * 2 * width, 2 * width)
        return pltpu.make_async_copy(x_hbm.at[rows], x.at[rows], x_sem.at[b])

    def y_copy(c, h):
        cols = pl.ds(pl.multiple_of(((me * chunks + c) * 2 + h) * width, width), width)
        return pltpu.make_async_copy(y_ref.at[:, cols], res.at[me * chunks + c, pl.ds(8 * h, 8)], y_sem.at[c * 2 + h])

    def rs_copy(rel, c):
        return pltpu.make_async_remote_copy(
            src_ref=upd.at[peer(rel) * chunks + c], dst_ref=inbox.at[c, back(rel)],
            send_sem=rs_send.at[rel, c], recv_sem=rs_recv.at[back(rel), c],
            device_id={"feat": peer(rel)}, device_id_type=MESH)

    def rs_arrival(rel, c):
        return pltpu.make_async_remote_copy(
            src_ref=upd.at[peer(rel) * chunks + c], dst_ref=inbox.at[c, rel],
            send_sem=rs_send.at[rel, c], recv_sem=rs_recv.at[rel, c],
            device_id={"feat": peer(rel)}, device_id_type=MESH)

    def ag_copy(rel, c):
        own = res.at[me * chunks + c]
        return pltpu.make_async_remote_copy(
            src_ref=own, dst_ref=own, send_sem=ag_send.at[rel, c], recv_sem=ag_recv.at[back(rel), c],
            device_id={"feat": peer(rel)}, device_id_type=MESH)

    def fw_copy(rel, c):
        block = res.at[peer(rel) * chunks + c]
        return pltpu.make_async_remote_copy(
            src_ref=block, dst_ref=block, send_sem=fw_send.at[rel // 2, c], recv_sem=ag_recv.at[rel + 1, c],
            device_id={"feat": peer(1)}, device_id_type=MESH)

    def ag_arrival(rel, c):
        block = res.at[peer(rel) * chunks + c]
        return pltpu.make_async_remote_copy(
            src_ref=block, dst_ref=block, send_sem=ag_send.at[rel, c], recv_sem=ag_recv.at[rel, c],
            device_id={"feat": peer(rel)}, device_id_type=MESH)

    def x_pair(b):
        start = pl.multiple_of(b * (2 * width), 2 * width)
        return x[pl.ds(start, width)], x[pl.ds(start + width, width)]

    def two_by_two(coef):
        zero = jnp.zeros_like(coef)
        top = jnp.concatenate([coef, zero], axis=1)
        low = jnp.concatenate([zero, coef], axis=1)
        return jnp.concatenate([top, low], axis=0).astype(jnp.bfloat16)

    def block_product(lhs, b):
        return jnp.dot(lhs, xt[b], preferred_element_type=jnp.float32).astype(jnp.bfloat16)

    def gradient_term(resid, b):
        first, second = x_pair(b)
        return jnp.dot(resid.astype(jnp.bfloat16), jnp.concatenate([first, second], axis=1),
                       preferred_element_type=jnp.float32)

    def gradient_of(acc):
        half = acc.shape[1] // 2
        return (acc[:8, :half] + acc[8:, half:]) * (1.0 / samples)

    def scatter(product):
        pending = None
        for rel in sends:
            for c in range(chunks):
                b = peer(rel) * chunks + c
                upd[b] = product(b)
                if pending is not None:
                    rs_copy(*pending).start()
                pending = (rel, c)
        for c in range(chunks):
            inbox[c, 0] = product(me * chunks + c)
            if pending is not None:
                rs_copy(*pending).start()
                pending = None

    def sum_and_gather(scale):
        for c in range(chunks):
            total = inbox[c, 0].astype(jnp.float32)
            for rel in sends[::-1]:
                rs_arrival(rel, c).wait_recv()
                total = total + inbox[c, rel].astype(jnp.float32)
            b = me * chunks + c
            res[b] = res[b] - scale * total
            for rel in far_first + [1]:
                ag_copy(rel, c).start()

    def gather_arrivals(use):
        late = []
        for c in range(chunks):
            for rel in direct:
                ag_arrival(rel, c).wait_recv()
                if rel != 1:
                    fw_copy(rel, c).start()
                use(rel, c)
            for rel, k in late:
                ag_arrival(rel, k).wait_recv()
                use(rel, k)
            late = [(rel + 1, c) for rel in near]
        for rel, k in late:
            ag_arrival(rel, k).wait_recv()
            use(rel, k)

    def wait_sends():
        for c in range(chunks):
            for rel in sends:
                rs_copy(rel, c).wait_send()
            for rel in direct:
                ag_copy(rel, c).wait_send()
            for rel in near:
                fw_copy(rel, c).wait_send()

    for b in range(blocks):
        x_copy(b).start()
    for c in range(chunks):
        for h in (0, 1):
            y_copy(c, h).start()

    barrier = pltpu.get_barrier_semaphore()
    for rel in range(1, group):
        pl.semaphore_signal(barrier, inc=1, device_id={"feat": peer(rel)}, device_id_type=MESH)
    pl.semaphore_wait(barrier, group - 1)

    for b in range(blocks):
        x_copy(b).wait()
    weights = w_ref[...]
    start_lhs = two_by_two(weights)

    def first_product(b):
        first, second = x_pair(b)
        rows = jnp.concatenate([first, second], axis=1)
        full = lax.dot_general(start_lhs, rows, (((1,), (1,)), ((), ())), preferred_element_type=jnp.float32)
        return full.astype(jnp.bfloat16)

    scatter(first_product)

    def prepare(b, total):
        first, second = x_pair(b)
        half = first.shape[1]
        xt[b, :half] = first.T
        xt[b, half:] = second.T
        both = first.astype(jnp.float32), second.astype(jnp.float32)
        for part in both:
            square = part * part
            total = total + jnp.sum(square.reshape(width // 8, 8, half), axis=0)
        return total

    squares = lax.fori_loop(0, blocks, prepare, jnp.zeros((8, x.shape[1]), jnp.float32))
    step_size = samples / (group * jnp.sum(squares))

    for c in range(chunks):
        for h in (0, 1):
            y_copy(c, h).wait()
    sum_and_gather(1.0)

    def sweep(sweep_idx, weights):
        acc = [jnp.zeros((16, 2 * x.shape[1]), jnp.float32)]
        for c in range(chunks):
            b = me * chunks + c
            acc[0] = acc[0] + gradient_term(res[b], b)

        def use(rel, c):
            b = peer(rel) * chunks + c
            acc[0] = acc[0] + gradient_term(res[b], b)

        gather_arrivals(use)
        coef = step_size * (gradient_of(acc[0]) - RIDGE * weights)
        for step_idx in range(1, LOCAL_STEPS):
            lhs = two_by_two(coef)
            total = jnp.zeros((16, 2 * x.shape[1]), jnp.float32)
            for b in range(blocks):
                product = block_product(lhs, b).astype(jnp.float32)
                total = total + gradient_term(res[b] - group * product, b)
            coef = coef + step_size * (gradient_of(total) - RIDGE * (weights + coef))
        lhs = two_by_two(coef)
        wait_sends()
        scatter(lambda b: block_product(lhs, b))
        sum_and_gather(GAMMA)
        return weights + GAMMA * coef

    w_out[...] = lax.fori_loop(0, SWEEPS, sweep, weights)

    def out_copy(rel, c, h):
        b = peer(rel) * chunks + c
        cols = pl.ds(pl.multiple_of((b * 2 + h) * width, width), width)
        return pltpu.make_async_copy(res.at[b, pl.ds(8 * h, 8)], r_out.at[:, cols], o_sem.at[rel, c * 2 + h])

    def put(rel, c):
        for h in (0, 1):
            out_copy(rel, c, h).start()

    for c in range(chunks):
        put(0, c)
    gather_arrivals(put)
    wait_sends()
    for rel in range(group):
        for c in range(chunks):
            for h in (0, 1):
                out_copy(rel, c, h).wait()


def solution(mesh):
    group = mesh.shape["feat"]

    def per_device(design, w_init, targets):
        samples, feats = design.shape
        outs = targets.shape[1]
        chunks = samples // (2 * LANES * group)
        blocks = group * chunks
        any_space = pl.BlockSpec(memory_space=pl.ANY)
        vmem = pl.BlockSpec(memory_space=pltpu.VMEM)
        weights, residual = pl.pallas_call(
            functools.partial(kernel, group, chunks),
            out_shape=(jax.ShapeDtypeStruct((outs, feats), jnp.float32),
                       jax.ShapeDtypeStruct((outs, samples), jnp.float32)),
            in_specs=[any_space, vmem, any_space],
            out_specs=(vmem, any_space),
            scratch_shapes=[
                pltpu.VMEM((samples, feats), jnp.bfloat16),
                pltpu.VMEM((blocks, 2 * feats, LANES), jnp.bfloat16),
                pltpu.VMEM((blocks, 2 * outs, LANES), jnp.float32),
                pltpu.VMEM((blocks, 2 * outs, LANES), jnp.bfloat16),
                pltpu.VMEM((chunks, group, 2 * outs, LANES), jnp.bfloat16),
                pltpu.SemaphoreType.DMA((blocks,)),
                pltpu.SemaphoreType.DMA((2 * chunks,)),
                pltpu.SemaphoreType.DMA((group, 2 * chunks)),
                pltpu.SemaphoreType.DMA((group, chunks)),
                pltpu.SemaphoreType.DMA((group, chunks)),
                pltpu.SemaphoreType.DMA((group, chunks)),
                pltpu.SemaphoreType.DMA((group, chunks)),
                pltpu.SemaphoreType.DMA((group // 2, chunks)),
            ],
            compiler_params=pltpu.CompilerParams(collective_id=0, has_side_effects=True,
                                                 vmem_limit_bytes=48 * 1024 * 1024),
        )(design, w_init.T, targets.T)
        return weights.T, residual.T

    return jax.shard_map(
        per_device,
        mesh=mesh,
        in_specs=(P(None, ("prob", "feat")), P(("prob", "feat"), None), P("prob", None)),
        out_specs=(P(("prob", "feat"), None), P("prob", None)),
        check_vma=False,
    )
```

```python
import functools

import jax
import jax.numpy as jnp
from jax import lax
from jax.experimental import pallas as pl
from jax.experimental.pallas import tpu as pltpu
from jax.sharding import PartitionSpec as P

LOCAL_STEPS = 2
SWEEPS = 6
RIDGE = 0.01
GAMMA = 0.75

LANES = 512
CHUNKS = (1, 1, 1, 1)
AHEAD = 1
MESH = pl.DeviceIdType.MESH


def kernel(group, per_owner, x_hbm, w_hbm, y_hbm, w_out, r_out,
           x, xt, w_in, res, upd, inbox,
           x_sem, w_sem, y_sem, rs_send, rs_recv, ag_send, ag_recv, fw_send):
    chips = group // 2
    width = LANES
    blocks = chips * per_owner
    samples, feats = x.shape
    me = lax.axis_index("feat")
    chip, core = me // 2, me % 2

    others = sorted(range(1, chips), key=lambda d: -min(d, chips - d))
    everyone = others + [0]
    chunks = []
    for count in CHUNKS:
        chunks.append((sum(n for _, n in chunks), count))
    assert sum(CHUNKS) == per_owner

    def owner(d):
        return (chip + d) % chips

    def on_owner(body):
        pl.when(core == 1)(body)

    def on_helper(body):
        pl.when(core == 0)(body)

    def span(d, c):
        start, count = chunks[c]
        return pl.ds(owner(d) * per_owner + start, count)

    def blocks_of(d, c):
        start, count = chunks[c]
        return [owner(d) * per_owner + start + k for k in range(count)]

    def x_copy(d, c):
        start, count = chunks[c]
        rows = pl.ds(pl.multiple_of((owner(d) * per_owner + start) * 2 * width, 2 * width), count * 2 * width)
        return pltpu.make_async_copy(x_hbm.at[rows], x.at[rows], x_sem.at[d, c])

    def y_copy(k, h):
        b = chip * per_owner + k
        cols = pl.ds(pl.multiple_of((b * 2 + h) * width, width), width)
        return pltpu.make_async_copy(y_hbm.at[:, cols], res.at[b, pl.ds(8 * h, 8)], y_sem.at[k * 2 + h])

    def remote(src, dst, send, recv, chip_to, core_to):
        return pltpu.make_async_remote_copy(src_ref=src, dst_ref=dst, send_sem=send, recv_sem=recv,
                                            device_id={"feat": chip_to * 2 + core_to}, device_id_type=MESH)

    def rs_copy(d, c):
        slot = (chips - d) % chips * 2 + core
        start, count = chunks[c]
        return remote(upd.at[span(d, c)], inbox.at[slot, pl.ds(start, count)],
                      rs_send.at[d, c], rs_recv.at[slot, c], owner(d), 1)

    def rs_arrival(slot, c):
        start, count = chunks[c]
        return remote(upd.at[span(0, c)], inbox.at[slot, pl.ds(start, count)],
                      rs_send.at[0, c], rs_recv.at[slot, c], owner(slot // 2), 1)

    def ag_copy(d, c):
        own = res.at[span(0, c)]
        return remote(own, own, ag_send.at[d, c], ag_recv.at[(chips - d) % chips, c], owner(d), 1)

    def fw_copy(d, c):
        part = res.at[span(d, c)]
        return remote(part, part, fw_send.at[d, c], ag_recv.at[d, c], chip, 0)

    def ag_arrival(d, c):
        part = res.at[span(d, c)]
        return remote(part, part, fw_send.at[d, c], ag_recv.at[d, c], chip, 0)

    def x_pair(b):
        start = pl.multiple_of(b * (2 * width), 2 * width)
        return x[pl.ds(start, width)], x[pl.ds(start + width, width)]

    def two_by_two(coef):
        zero = jnp.zeros_like(coef)
        top = jnp.concatenate([coef, zero], axis=1)
        low = jnp.concatenate([zero, coef], axis=1)
        return jnp.concatenate([top, low], axis=0).astype(jnp.bfloat16)

    def block_product(lhs, b):
        return jnp.dot(lhs, xt[b], preferred_element_type=jnp.float32).astype(jnp.bfloat16)

    def gradient_term(resid, b):
        return jnp.dot(resid.astype(jnp.bfloat16), jnp.concatenate(x_pair(b), axis=1),
                       preferred_element_type=jnp.float32)

    def gradient_of(acc):
        return (acc[:8, :feats] + acc[8:, feats:]) * (1.0 / samples)

    def scatter(product, ready=None):
        def compute(c):
            if ready is not None:
                ready(c)
            return [[product(b) for b in blocks_of(d, c)] for d in everyone]

        values = compute(0)
        for c in range(len(chunks)):
            for d, parts in zip(everyone, values):
                for b, part in zip(blocks_of(d, c), parts):
                    upd[b] = part
            if c + 1 < len(chunks):
                values = compute(c + 1)
            for d in others:
                rs_copy(d, c).start()
            on_helper(lambda: rs_copy(0, c).start())

    def sum_and_gather(scale):
        def body():
            for c in range(len(chunks)):
                for slot in range(group):
                    if slot != 1:
                        rs_arrival(slot, c).wait_recv()
                start, count = chunks[c]
                for k in range(start, start + count):
                    b = chip * per_owner + k
                    total = upd[b].astype(jnp.float32)
                    for slot in range(group):
                        if slot != 1:
                            total = total + inbox[slot, k].astype(jnp.float32)
                    res[b] = res[b] - scale * total
                for d in others:
                    ag_copy(d, c).start()
                fw_copy(0, c).start()
        on_owner(body)

    def gather_arrivals(use):
        for c in range(len(chunks)):
            on_helper(lambda: ag_arrival(0, c).wait_recv())
            for d in others[::-1]:
                ag_arrival(d, c).wait_recv()
                on_owner(lambda: fw_copy(d, c).start())
            use([b for d in everyone for b in blocks_of(d, c)])

    def wait_sends():
        for c in range(len(chunks)):
            for d in others:
                rs_copy(d, c).wait_send()

        def helper():
            for c in range(len(chunks)):
                rs_copy(0, c).wait_send()

        def owning():
            for c in range(len(chunks)):
                for d in others:
                    ag_copy(d, c).wait_send()
                for d in everyone:
                    fw_copy(d, c).wait_send()

        on_helper(helper)
        on_owner(owning)

    w_copy = pltpu.make_async_copy(w_hbm, w_in, w_sem)
    w_copy.start()
    for c in range(len(chunks)):
        for d in everyone:
            x_copy(d, c).start()

    def load_targets():
        for k in range(per_owner):
            for h in (0, 1):
                y_copy(k, h).start()
        for k in range(per_owner):
            for h in (0, 1):
                y_copy(k, h).wait()

    barrier = pltpu.get_barrier_semaphore()
    for step in range(1, group):
        pl.semaphore_signal(barrier, inc=1, device_id={"feat": (me + step) % group}, device_id_type=MESH)
    w_copy.wait()
    weights = w_in[...]
    start_lhs = two_by_two(weights)
    pl.semaphore_wait(barrier, group - 1)

    def first_product(b):
        rows = jnp.concatenate(x_pair(b), axis=1)
        full = lax.dot_general(start_lhs, rows, (((1,), (1,)), ((), ())), preferred_element_type=jnp.float32)
        return full.astype(jnp.bfloat16)

    def x_ready(c):
        for d in everyone:
            x_copy(d, c).wait()

    scatter(first_product, x_ready)
    on_owner(load_targets)

    def prepare(b, total):
        first, second = x_pair(b)
        xt[b, :feats] = first.T
        xt[b, feats:] = second.T
        for part in (first.astype(jnp.float32), second.astype(jnp.float32)):
            total = total + jnp.sum((part * part).reshape(width // 8, 8, feats), axis=0)
        return total

    squares = jnp.zeros((8, feats), jnp.float32)
    squares = lax.fori_loop(0, blocks // 2, prepare, squares)
    sum_and_gather(1.0)
    squares = lax.fori_loop(blocks // 2, blocks, prepare, squares)
    step_size = samples / (group * jnp.sum(squares))

    def sweep(sweep_idx, weights):
        acc = [jnp.zeros((16, 2 * feats), jnp.float32)]

        def use(parts):
            for b in parts:
                acc[0] = acc[0] + gradient_term(res[b], b)

        gather_arrivals(use)
        coef = step_size * (gradient_of(acc[0]) - RIDGE * weights)
        for step_idx in range(1, LOCAL_STEPS):
            lhs = two_by_two(coef)
            total = jnp.zeros((16, 2 * feats), jnp.float32)
            queue = [block_product(lhs, b) for b in range(AHEAD)]
            for b in range(blocks):
                if b + AHEAD < blocks:
                    queue.append(block_product(lhs, b + AHEAD))
                product = queue.pop(0).astype(jnp.float32)
                total = total + gradient_term(res[b] - group * product, b)
            coef = coef + step_size * (gradient_of(total) - RIDGE * (weights + coef))
        lhs = two_by_two(coef)
        wait_sends()
        scatter(lambda b: block_product(lhs, b))
        sum_and_gather(GAMMA)
        return weights + GAMMA * coef

    w_out[...] = lax.fori_loop(0, SWEEPS, sweep, weights)

    def put(parts):
        for b in parts:
            for h in (0, 1):
                cols = pl.ds(pl.multiple_of((b * 2 + h) * width, width), width)
                r_out[:, cols] = res[b, 8 * h:8 * h + 8]

    gather_arrivals(put)
    wait_sends()


def solution(mesh):
    group = mesh.shape["feat"]

    def per_device(design, w_init, targets):
        samples, feats = design.shape
        outs = targets.shape[1]
        chips = group // 2
        per_owner = samples // (2 * LANES * chips)
        blocks = chips * per_owner
        parts = len(CHUNKS)
        hbm = pl.BlockSpec(memory_space=pltpu.HBM)
        vmem = pl.BlockSpec(memory_space=pltpu.VMEM)
        dma = pltpu.SemaphoreType.DMA
        weights, residual = pl.pallas_call(
            functools.partial(kernel, group, per_owner),
            out_shape=(jax.ShapeDtypeStruct((outs, feats), jnp.float32),
                       jax.ShapeDtypeStruct((outs, samples), jnp.float32)),
            in_specs=[hbm, hbm, hbm],
            out_specs=(vmem, vmem),
            scratch_shapes=[
                pltpu.VMEM((samples, feats), jnp.bfloat16),
                pltpu.VMEM((blocks, 2 * feats, LANES), jnp.bfloat16),
                pltpu.VMEM((outs, feats), jnp.float32),
                pltpu.VMEM((blocks, 2 * outs, LANES), jnp.float32),
                pltpu.VMEM((blocks, 2 * outs, LANES), jnp.bfloat16),
                pltpu.VMEM((group, per_owner, 2 * outs, LANES), jnp.bfloat16),
                dma((chips, parts)),
                dma,
                dma((2 * per_owner,)),
                dma((chips, parts)),
                dma((group, parts)),
                dma((chips, parts)),
                dma((chips, parts)),
                dma((chips, parts)),
            ],
            compiler_params=pltpu.CompilerParams(collective_id=0, has_side_effects=True,
                                                 vmem_limit_bytes=67043328),
        )(design, w_init.T, targets.T)
        return weights.T, residual.T

    return jax.shard_map(
        per_device,
        mesh=mesh,
        in_specs=(P(None, ("prob", "feat")), P(("prob", "feat"), None), P("prob", None)),
        out_specs=(P(("prob", "feat"), None), P("prob", None)),
        check_vma=False,
    )
```

```python
import functools

import jax
import jax.numpy as jnp
from jax import lax
from jax.experimental import pallas as pl
from jax.experimental.pallas import tpu as pltpu
from jax.sharding import PartitionSpec as P

LOCAL_STEPS = 2
SWEEPS = 6
RIDGE = 0.01
GAMMA = 0.75

LANES = 256
PARTS = 4
CHUNKS = (2, 2)
AHEAD = 1
MESH = pl.DeviceIdType.MESH


def kernel(group, per_owner, x_hbm, w_in, y_hbm, w_out, r_out,
           x, xt, y_in, res, upd, inbox,
           x_sem, y_sem, rs_send, rs_recv, ag_send, ag_recv, fw_send):
    chips = group // 2
    width = LANES
    blocks = chips * per_owner
    samples, feats = x.shape
    rows = w_in.shape[0] // 2
    size = PARTS * width
    halves = (0, 1)
    me = lax.axis_index("feat")
    chip, core = me // 2, me % 2

    others = sorted(range(1, chips), key=lambda d: -min(d, chips - d))
    everyone = others + [0]
    chunks = []
    for count in CHUNKS:
        chunks.append((sum(n for _, n in chunks), count))
    assert sum(CHUNKS) == per_owner

    def owner(d):
        return (chip + d) % chips

    def on_owner(body):
        pl.when(core == 1)(body)

    def on_helper(body):
        pl.when(core == 0)(body)

    def span(d, c):
        start, count = chunks[c]
        return pl.ds(owner(d) * per_owner + start, count)

    def blocks_of(d, c):
        start, count = chunks[c]
        return [owner(d) * per_owner + start + k for k in range(count)]

    def x_copy(d, c):
        start, count = chunks[c]
        part = pl.ds(pl.multiple_of((owner(d) * per_owner + start) * size, size), count * size)
        return pltpu.make_async_copy(x_hbm.at[part], x.at[part], x_sem.at[d, c])

    def y_copy():
        cols = pl.ds(pl.multiple_of(chip * (per_owner * size), per_owner * size), per_owner * size)
        return pltpu.make_async_copy(y_hbm.at[:, cols], y_in, y_sem)

    def remote(src, dst, send, recv, chip_to, core_to):
        return pltpu.make_async_remote_copy(src_ref=src, dst_ref=dst, send_sem=send, recv_sem=recv,
                                            device_id={"feat": chip_to * 2 + core_to}, device_id_type=MESH)

    def rs_copy(p, d, c):
        slot = (chips - d) % chips * 2 + core
        start, count = chunks[c]
        return remote(upd.at[p, span(d, c)], inbox.at[p, slot, pl.ds(start, count)],
                      rs_send.at[p, d, c], rs_recv.at[p, slot, c], owner(d), 1)

    def rs_arrival(p, slot, c):
        start, count = chunks[c]
        return remote(upd.at[p, span(0, c)], inbox.at[p, slot, pl.ds(start, count)],
                      rs_send.at[p, 0, c], rs_recv.at[p, slot, c], owner(slot // 2), 1)

    def ag_copy(p, d, c):
        own = res.at[p, span(0, c)]
        return remote(own, own, ag_send.at[p, d, c], ag_recv.at[p, (chips - d) % chips, c], owner(d), 1)

    def fw_copy(p, d, c):
        part = res.at[p, span(d, c)]
        return remote(part, part, fw_send.at[p, d, c], ag_recv.at[p, d, c], chip, 0)

    def x_parts(b):
        start = pl.multiple_of(b * size, size)
        return [x[pl.ds(start + q * width, width)] for q in range(PARTS)]

    def diagonal(coef):
        tall = jnp.concatenate([coef] * PARTS, axis=0)
        place = lax.broadcasted_iota(jnp.int32, tall.shape, 0) // rows
        return jnp.concatenate([jnp.where(place == q, tall, 0.0) for q in range(PARTS)], axis=1).astype(jnp.bfloat16)

    def block_product(lhs, b):
        return jnp.dot(lhs, xt[b], preferred_element_type=jnp.float32).astype(jnp.bfloat16)

    def gradient_term(resid, b):
        return jnp.dot(resid.astype(jnp.bfloat16), jnp.concatenate(x_parts(b), axis=1),
                       preferred_element_type=jnp.float32)

    def gradient_of(acc):
        total = acc[:rows, :feats]
        for q in range(1, PARTS):
            total = total + acc[q * rows:(q + 1) * rows, q * feats:(q + 1) * feats]
        return total * (1.0 / samples)

    def send_chunk(p, c):
        for d in others:
            rs_copy(p, d, c).start()
        on_helper(lambda: rs_copy(p, 0, c).start())

    def scatter(p, lhs):
        for c in range(len(chunks)):
            values = [(b, block_product(lhs, b)) for d in everyone for b in blocks_of(d, c)]
            for b, value in values:
                upd[p, b] = value
            send_chunk(p, c)

    def sum_and_gather(p, scale):
        def body():
            for c in range(len(chunks)):
                for slot in range(group):
                    if slot != 1:
                        rs_arrival(p, slot, c).wait_recv()
                start, count = chunks[c]
                for k in range(start, start + count):
                    b = chip * per_owner + k
                    total = upd[p, b].astype(jnp.float32)
                    for slot in range(group):
                        if slot != 1:
                            total = total + inbox[p, slot, k].astype(jnp.float32)
                    res[p, b] = res[p, b] - scale * total
                for d in others:
                    ag_copy(p, d, c).start()
                fw_copy(p, 0, c).start()
        on_owner(body)

    def gather_arrivals(p, use, early=False):
        for c in range(len(chunks)):
            if early and c == len(chunks) - 1:
                wait_scatter(p)
            on_helper(lambda: fw_copy(p, 0, c).wait_recv())
            for d in others[::-1]:
                fw_copy(p, d, c).wait_recv()
                on_owner(lambda: fw_copy(p, d, c).start())
            use([b for d in everyone for b in blocks_of(d, c)])

    def wait_scatter(p):
        for c in range(len(chunks)):
            for d in others:
                rs_copy(p, d, c).wait_send()

        def helper():
            for c in range(len(chunks)):
                rs_copy(p, 0, c).wait_send()

        on_helper(helper)

    def wait_gather(p):
        def owning():
            for c in range(len(chunks)):
                for d in others:
                    ag_copy(p, d, c).wait_send()
                for d in everyone:
                    fw_copy(p, d, c).wait_send()
        on_owner(owning)

    for c in range(len(chunks)):
        for d in everyone:
            x_copy(d, c).start()
    on_owner(lambda: y_copy().start())

    barrier = pltpu.get_barrier_semaphore()
    for step in range(1, group):
        pl.semaphore_signal(barrier, inc=1, device_id={"feat": (me + step) % group}, device_id_type=MESH)
    start_weights = tuple(w_in[p * rows:(p + 1) * rows] for p in halves)
    start_lhs = jnp.concatenate([diagonal(start_weights[p]) for p in halves], axis=0)

    for c in range(len(chunks)):
        for d in everyone:
            x_copy(d, c).wait()
        for b in [b for d in everyone for b in blocks_of(d, c)]:
            both = lax.dot_general(start_lhs, jnp.concatenate(x_parts(b), axis=1), (((1,), (1,)), ((), ())),
                                   preferred_element_type=jnp.float32).astype(jnp.bfloat16)
            for p in halves:
                upd[p, b] = both[p * PARTS * rows:(p + 1) * PARTS * rows]
        if c == 0:
            pl.semaphore_wait(barrier, group - 1)
        send_chunk(0, c)
    for c in range(len(chunks)):
        send_chunk(1, c)

    def prepare(b, total):
        for q, part in enumerate(x_parts(b)):
            xt[b, q * feats:(q + 1) * feats] = part.T
            wide = part.astype(jnp.float32)
            total = total + jnp.sum((wide * wide).reshape(width // 8, 8, feats), axis=0)
        return total

    squares = jnp.zeros((8, feats), jnp.float32)
    squares = lax.fori_loop(0, blocks // 2, prepare, squares)

    def take_targets():
        y_copy().wait()
        for p in halves:
            for k in range(per_owner):
                res[p, chip * per_owner + k] = jnp.concatenate(
                    [y_in[p * rows:(p + 1) * rows, (k * PARTS + q) * width:(k * PARTS + q + 1) * width]
                     for q in range(PARTS)], axis=0)

    on_owner(take_targets)
    for p in halves:
        sum_and_gather(p, 1.0)
    squares = lax.fori_loop(blocks // 2, blocks, prepare, squares)
    step_size = samples / (group * jnp.sum(squares))

    def half_sweep(p, weights):
        acc = [jnp.zeros((PARTS * rows, PARTS * feats), jnp.float32)]

        def use(parts):
            for b in parts:
                acc[0] = acc[0] + gradient_term(res[p, b], b)

        gather_arrivals(p, use, True)
        coef = step_size * (gradient_of(acc[0]) - RIDGE * weights)
        for step_idx in range(1, LOCAL_STEPS):
            lhs = diagonal(coef)
            total = jnp.zeros((PARTS * rows, PARTS * feats), jnp.float32)
            queue = [block_product(lhs, b) for b in range(AHEAD)]
            for b in range(blocks):
                if b + AHEAD < blocks:
                    queue.append(block_product(lhs, b + AHEAD))
                product = queue.pop(0).astype(jnp.float32)
                total = total + gradient_term(res[p, b] - group * product, b)
            coef = coef + step_size * (gradient_of(total) - RIDGE * (weights + coef))
        wait_gather(p)
        scatter(p, diagonal(coef))
        return weights + GAMMA * coef

    def sweep(sweep_idx, weights):
        weights = tuple(half_sweep(p, weights[p]) for p in halves)
        for p in halves:
            sum_and_gather(p, GAMMA)
        return weights

    end_weights = lax.fori_loop(0, SWEEPS, sweep, start_weights)
    for p in halves:
        w_out[p * rows:(p + 1) * rows] = end_weights[p]

        def put(parts):
            for b in parts:
                for q in range(PARTS):
                    cols = pl.ds(pl.multiple_of((b * PARTS + q) * width, width), width)
                    r_out[p * rows:(p + 1) * rows, cols] = res[p, b, q * rows:(q + 1) * rows]

        gather_arrivals(p, put)
        wait_scatter(p)
        wait_gather(p)


def solution(mesh):
    group = mesh.shape["feat"]

    def per_device(design, w_init, targets):
        samples, feats = design.shape
        outs = targets.shape[1]
        chips = group // 2
        blocks = samples // (PARTS * LANES)
        per_owner = blocks // chips
        parts = len(CHUNKS)
        rows = PARTS * outs // 2
        hbm = pl.BlockSpec(memory_space=pltpu.HBM)
        vmem = pl.BlockSpec(memory_space=pltpu.VMEM)
        dma = pltpu.SemaphoreType.DMA
        weights, residual = pl.pallas_call(
            functools.partial(kernel, group, per_owner),
            out_shape=(jax.ShapeDtypeStruct((outs, feats), jnp.float32),
                       jax.ShapeDtypeStruct((outs, samples), jnp.float32)),
            in_specs=[hbm, vmem, hbm],
            out_specs=(vmem, vmem),
            scratch_shapes=[
                pltpu.VMEM((samples, feats), jnp.bfloat16),
                pltpu.VMEM((blocks, PARTS * feats, LANES), jnp.bfloat16),
                pltpu.VMEM((outs, per_owner * PARTS * LANES), jnp.float32),
                pltpu.VMEM((2, blocks, rows, LANES), jnp.float32),
                pltpu.VMEM((2, blocks, rows, LANES), jnp.bfloat16),
                pltpu.VMEM((2, group, per_owner, rows, LANES), jnp.bfloat16),
                dma((chips, parts)),
                dma,
                dma((2, chips, parts)),
                dma((2, group, parts)),
                dma((2, chips, parts)),
                dma((2, chips, parts)),
                dma((2, chips, parts)),
            ],
            compiler_params=pltpu.CompilerParams(collective_id=0, has_side_effects=True,
                                                 vmem_limit_bytes=56000000),
        )(design, w_init.T, targets.T)
        return weights.T, residual.T

    return jax.shard_map(
        per_device,
        mesh=mesh,
        in_specs=(P(None, ("prob", "feat")), P(("prob", "feat"), None), P("prob", None)),
        out_specs=(P(("prob", "feat"), None), P("prob", None)),
        check_vma=False,
    )
```

```python
import functools

import jax
import jax.numpy as jnp
from jax import lax
from jax.experimental import pallas as pl
from jax.experimental.pallas import tpu as pltpu
from jax.sharding import PartitionSpec as P

LOCAL_STEPS = 2
SWEEPS = 6
RIDGE = 0.01
GAMMA = 0.75

LANES = 256
PARTS = 4
CHUNKS = (2, 2)
AHEAD = 4
MESH = pl.DeviceIdType.MESH


def kernel(group, per_owner, x_hbm, w_in, y_hbm, w_out, r_out,
           x, xt, y_in, res, upd, inbox,
           x_sem, y_sem, rs_send, rs_recv, ag_send, ag_recv, fw_send):
    chips = group // 2
    width = LANES
    blocks = chips * per_owner
    samples, feats = x.shape
    rows = w_in.shape[0] // 2
    size = PARTS * width
    halves = (0, 1)
    me = lax.axis_index("feat")
    chip, core = me // 2, me % 2

    others = sorted(range(1, chips), key=lambda d: -min(d, chips - d))
    everyone = others + [0]
    chunks = []
    for count in CHUNKS:
        chunks.append((sum(n for _, n in chunks), count))
    assert sum(CHUNKS) == per_owner

    def owner(d):
        return (chip + d) % chips

    def on_owner(body):
        pl.when(core == 1)(body)

    def on_helper(body):
        pl.when(core == 0)(body)

    def span(d, c):
        start, count = chunks[c]
        return pl.ds(owner(d) * per_owner + start, count)

    def blocks_of(d, c):
        start, count = chunks[c]
        return [owner(d) * per_owner + start + k for k in range(count)]

    def x_copy(d, c):
        start, count = chunks[c]
        part = pl.ds(pl.multiple_of((owner(d) * per_owner + start) * size, size), count * size)
        return pltpu.make_async_copy(x_hbm.at[part], x.at[part], x_sem.at[d, c])

    def y_copy():
        cols = pl.ds(pl.multiple_of(chip * (per_owner * size), per_owner * size), per_owner * size)
        return pltpu.make_async_copy(y_hbm.at[:, cols], y_in, y_sem)

    def remote(src, dst, send, recv, chip_to, core_to):
        return pltpu.make_async_remote_copy(src_ref=src, dst_ref=dst, send_sem=send, recv_sem=recv,
                                            device_id={"feat": chip_to * 2 + core_to}, device_id_type=MESH)

    def rs_copy(p, d, c):
        slot = (chips - d) % chips * 2 + core
        start, count = chunks[c]
        return remote(upd.at[p, span(d, c)], inbox.at[p, slot, pl.ds(start, count)],
                      rs_send.at[p, d, c], rs_recv.at[p, slot, c], owner(d), 1)

    def rs_arrival(p, slot, c):
        start, count = chunks[c]
        return remote(upd.at[p, span(0, c)], inbox.at[p, slot, pl.ds(start, count)],
                      rs_send.at[p, 0, c], rs_recv.at[p, slot, c], owner(slot // 2), 1)

    def ag_copy(p, d, c):
        own = res.at[p, span(0, c)]
        return remote(own, own, ag_send.at[p, d, c], ag_recv.at[p, (chips - d) % chips, c], owner(d), 1)

    def fw_copy(p, d, c):
        part = res.at[p, span(d, c)]
        return remote(part, part, fw_send.at[p, d, c], ag_recv.at[p, d, c], chip, 0)

    def x_parts(b):
        start = pl.multiple_of(b * size, size)
        return [x[pl.ds(start + q * width, width)] for q in range(PARTS)]

    def diagonal(coef):
        tall = jnp.concatenate([coef] * PARTS, axis=0)
        place = lax.broadcasted_iota(jnp.int32, tall.shape, 0) // rows
        return jnp.concatenate([jnp.where(place == q, tall, 0.0) for q in range(PARTS)], axis=1).astype(jnp.bfloat16)

    def block_product(lhs, b):
        return jnp.dot(lhs, xt[b], preferred_element_type=jnp.float32).astype(jnp.bfloat16)

    def gradient_term(resid, b):
        return jnp.dot(resid.astype(jnp.bfloat16), jnp.concatenate(x_parts(b), axis=1),
                       preferred_element_type=jnp.float32)

    def gradient_of(acc):
        total = acc[:rows, :feats]
        for q in range(1, PARTS):
            total = total + acc[q * rows:(q + 1) * rows, q * feats:(q + 1) * feats]
        return total * (1.0 / samples)

    def send_chunk(p, c):
        for d in others:
            rs_copy(p, d, c).start()
        on_helper(lambda: rs_copy(p, 0, c).start())

    def scatter(p, lhs):
        for c in range(len(chunks)):
            values = [(b, block_product(lhs, b)) for d in everyone for b in blocks_of(d, c)]
            for b, value in values:
                upd[p, b] = value
            send_chunk(p, c)

    def sum_and_gather(p, scale):
        def body():
            for c in range(len(chunks)):
                for slot in range(group):
                    if slot != 1:
                        rs_arrival(p, slot, c).wait_recv()
                start, count = chunks[c]
                for k in range(start, start + count):
                    b = chip * per_owner + k
                    total = upd[p, b].astype(jnp.float32)
                    for slot in range(group):
                        if slot != 1:
                            total = total + inbox[p, slot, k].astype(jnp.float32)
                    res[p, b] = res[p, b] - scale * total
                for d in others:
                    ag_copy(p, d, c).start()
                fw_copy(p, 0, c).start()
        on_owner(body)

    def gather_arrivals(p, use, early=False):
        for c in range(len(chunks)):
            if early and c == len(chunks) - 1:
                wait_scatter(p)
            on_helper(lambda: fw_copy(p, 0, c).wait_recv())
            for d in others[::-1]:
                fw_copy(p, d, c).wait_recv()
                on_owner(lambda: fw_copy(p, d, c).start())
            use([b for d in everyone for b in blocks_of(d, c)])

    def wait_scatter(p):
        for c in range(len(chunks)):
            for d in others:
                rs_copy(p, d, c).wait_send()

        def helper():
            for c in range(len(chunks)):
                rs_copy(p, 0, c).wait_send()

        on_helper(helper)

    def wait_gather(p):
        def owning():
            for c in range(len(chunks)):
                for d in others:
                    ag_copy(p, d, c).wait_send()
                for d in everyone:
                    fw_copy(p, d, c).wait_send()
        on_owner(owning)

    for c in range(len(chunks)):
        for d in everyone:
            x_copy(d, c).start()
    on_owner(lambda: y_copy().start())

    barrier = pltpu.get_barrier_semaphore()
    for step in range(1, group):
        pl.semaphore_signal(barrier, inc=1, device_id={"feat": (me + step) % group}, device_id_type=MESH)
    start_weights = tuple(w_in[p * rows:(p + 1) * rows] for p in halves)
    start_lhs = jnp.concatenate([diagonal(start_weights[p]) for p in halves], axis=0)

    for c in range(len(chunks)):
        for d in everyone:
            x_copy(d, c).wait()
        for b in [b for d in everyone for b in blocks_of(d, c)]:
            both = lax.dot_general(start_lhs, jnp.concatenate(x_parts(b), axis=1), (((1,), (1,)), ((), ())),
                                   preferred_element_type=jnp.float32).astype(jnp.bfloat16)
            for p in halves:
                upd[p, b] = both[p * PARTS * rows:(p + 1) * PARTS * rows]
        if c == 0:
            pl.semaphore_wait(barrier, group - 1)
        send_chunk(0, c)
    for c in range(len(chunks)):
        send_chunk(1, c)

    def prepare(b, total):
        for q, part in enumerate(x_parts(b)):
            xt[b, q * feats:(q + 1) * feats] = part.T
            wide = part.astype(jnp.float32)
            total = total + jnp.sum((wide * wide).reshape(width // 8, 8, feats), axis=0)
        return total

    squares = jnp.zeros((8, feats), jnp.float32)
    squares = lax.fori_loop(0, blocks // 2, prepare, squares)

    def take_targets():
        y_copy().wait()
        for p in halves:
            for k in range(per_owner):
                res[p, chip * per_owner + k] = jnp.concatenate(
                    [y_in[p * rows:(p + 1) * rows, (k * PARTS + q) * width:(k * PARTS + q + 1) * width]
                     for q in range(PARTS)], axis=0)

    on_owner(take_targets)
    for p in halves:
        sum_and_gather(p, 1.0)
    squares = lax.fori_loop(blocks // 2, blocks, prepare, squares)
    step_size = samples / (group * jnp.sum(squares))

    def half_sweep(p, weights):
        acc = [jnp.zeros((PARTS * rows, PARTS * feats), jnp.float32)]

        def use(parts):
            for b in parts:
                acc[0] = acc[0] + gradient_term(res[p, b], b)

        gather_arrivals(p, use, True)
        coef = step_size * (gradient_of(acc[0]) - RIDGE * weights)
        for step_idx in range(1, LOCAL_STEPS):
            lhs = diagonal(coef)
            total = jnp.zeros((PARTS * rows, PARTS * feats), jnp.float32)
            queue = [block_product(lhs, b) for b in range(AHEAD)]
            for b in range(blocks):
                if b + AHEAD < blocks:
                    queue.append(block_product(lhs, b + AHEAD))
                product = queue.pop(0).astype(jnp.float32)
                total = total + gradient_term(res[p, b] - group * product, b)
            coef = coef + step_size * (gradient_of(total) - RIDGE * (weights + coef))
        wait_gather(p)
        scatter(p, diagonal(coef))
        return weights + GAMMA * coef

    def sweep(sweep_idx, weights):
        weights = tuple(half_sweep(p, weights[p]) for p in halves)
        for p in halves:
            sum_and_gather(p, GAMMA)
        return weights

    end_weights = lax.fori_loop(0, SWEEPS, sweep, start_weights)
    for p in halves:
        w_out[p * rows:(p + 1) * rows] = end_weights[p]

        def put(parts):
            for b in parts:
                for q in range(PARTS):
                    cols = pl.ds(pl.multiple_of((b * PARTS + q) * width, width), width)
                    r_out[p * rows:(p + 1) * rows, cols] = res[p, b, q * rows:(q + 1) * rows]

        gather_arrivals(p, put)
        wait_scatter(p)
        wait_gather(p)


def solution(mesh):
    group = mesh.shape["feat"]

    def per_device(design, w_init, targets):
        samples, feats = design.shape
        outs = targets.shape[1]
        chips = group // 2
        blocks = samples // (PARTS * LANES)
        per_owner = blocks // chips
        parts = len(CHUNKS)
        rows = PARTS * outs // 2
        hbm = pl.BlockSpec(memory_space=pltpu.HBM)
        vmem = pl.BlockSpec(memory_space=pltpu.VMEM)
        dma = pltpu.SemaphoreType.DMA
        weights, residual = pl.pallas_call(
            functools.partial(kernel, group, per_owner),
            out_shape=(jax.ShapeDtypeStruct((outs, feats), jnp.float32),
                       jax.ShapeDtypeStruct((outs, samples), jnp.float32)),
            in_specs=[hbm, vmem, hbm],
            out_specs=(vmem, vmem),
            scratch_shapes=[
                pltpu.VMEM((samples, feats), jnp.bfloat16),
                pltpu.VMEM((blocks, PARTS * feats, LANES), jnp.bfloat16),
                pltpu.VMEM((outs, per_owner * PARTS * LANES), jnp.float32),
                pltpu.VMEM((2, blocks, rows, LANES), jnp.float32),
                pltpu.VMEM((2, blocks, rows, LANES), jnp.bfloat16),
                pltpu.VMEM((2, group, per_owner, rows, LANES), jnp.bfloat16),
                dma((chips, parts)),
                dma,
                dma((2, chips, parts)),
                dma((2, group, parts)),
                dma((2, chips, parts)),
                dma((2, chips, parts)),
                dma((2, chips, parts)),
            ],
            compiler_params=pltpu.CompilerParams(collective_id=0, has_side_effects=True,
                                                 vmem_limit_bytes=56000000),
        )(design, w_init.T, targets.T)
        return weights.T, residual.T

    return jax.shard_map(
        per_device,
        mesh=mesh,
        in_specs=(P(None, ("prob", "feat")), P(("prob", "feat"), None), P("prob", None)),
        out_specs=(P(("prob", "feat"), None), P("prob", None)),
        check_vma=False,
    )
```

```python
import functools

import jax
import jax.numpy as jnp
from jax import lax
from jax.experimental import pallas as pl
from jax.experimental.pallas import tpu as pltpu
from jax.sharding import PartitionSpec as P

LOCAL_STEPS = 2
SWEEPS = 6
RIDGE = 0.01
GAMMA = 0.75

LANES = 256
PARTS = 4
CHUNKS = (2, 2)
AHEAD = 4
MESH = pl.DeviceIdType.MESH


def kernel(group, per_owner, x_hbm, w_hbm, y_hbm, w_out, r_out,
           x, xt, w_in, w_sem, y_in, res, upd, inbox,
           x_sem, y_sem, rs_send, rs_recv, ag_send, ag_recv, fw_send):
    chips = group // 2
    width = LANES
    blocks = chips * per_owner
    samples, feats = x.shape
    rows = w_in.shape[0] // 2
    size = PARTS * width
    halves = (0, 1)
    me = lax.axis_index("feat")
    chip, core = me // 2, me % 2

    others = sorted(range(1, chips), key=lambda d: -min(d, chips - d))
    everyone = others + [0]
    chunks = []
    for count in CHUNKS:
        chunks.append((sum(n for _, n in chunks), count))
    assert sum(CHUNKS) == per_owner

    def owner(d):
        return (chip + d) % chips

    def on_owner(body):
        pl.when(core == 1)(body)

    def on_helper(body):
        pl.when(core == 0)(body)

    def span(d, c):
        start, count = chunks[c]
        return pl.ds(owner(d) * per_owner + start, count)

    def blocks_of(d, c):
        start, count = chunks[c]
        return [owner(d) * per_owner + start + k for k in range(count)]

    def x_copy(d, c):
        start, count = chunks[c]
        part = pl.ds(pl.multiple_of((owner(d) * per_owner + start) * size, size), count * size)
        return pltpu.make_async_copy(x_hbm.at[part], x.at[part], x_sem.at[d, c])

    def y_copy():
        cols = pl.ds(pl.multiple_of(chip * (per_owner * size), per_owner * size), per_owner * size)
        return pltpu.make_async_copy(y_hbm.at[:, cols], y_in, y_sem)

    def remote(src, dst, send, recv, chip_to, core_to):
        return pltpu.make_async_remote_copy(src_ref=src, dst_ref=dst, send_sem=send, recv_sem=recv,
                                            device_id={"feat": chip_to * 2 + core_to}, device_id_type=MESH)

    def rs_copy(p, d, c):
        slot = ((chips - d) % chips * 2 + 1 - core + group - 1) % group
        start, count = chunks[c]
        return remote(upd.at[p, span(d, c)], inbox.at[p, c, slot],
                      rs_send.at[p, d, c], rs_recv.at[p, c], owner(d), 1)

    def rs_arrivals(p, c):
        return remote(inbox.at[p, c], inbox.at[p, c], rs_send.at[p, 0, c], rs_recv.at[p, c], chip, 0)

    def ag_copy(p, d, c):
        own = res.at[p, span(0, c)]
        return remote(own, own, ag_send.at[p, d, c], ag_recv.at[p, (chips - d) % chips, c], owner(d), 1)

    def fw_copy(p, d, c):
        part = res.at[p, span(d, c)]
        return remote(part, part, fw_send.at[p, d, c], ag_recv.at[p, d, c], chip, 0)

    def x_parts(b):
        start = pl.multiple_of(b * size, size)
        return [x[pl.ds(start + q * width, width)] for q in range(PARTS)]

    def diagonal(coef):
        tall = jnp.concatenate([coef] * PARTS, axis=0)
        place = lax.broadcasted_iota(jnp.int32, tall.shape, 0) // rows
        return jnp.concatenate([jnp.where(place == q, tall, 0.0) for q in range(PARTS)], axis=1).astype(jnp.bfloat16)

    def block_product(lhs, b):
        return jnp.dot(lhs, xt[b], preferred_element_type=jnp.float32).astype(jnp.bfloat16)

    def gradient_term(resid, b):
        return jnp.dot(resid.astype(jnp.bfloat16), jnp.concatenate(x_parts(b), axis=1),
                       preferred_element_type=jnp.float32)

    def gradient_of(acc):
        total = acc[:rows, :feats]
        for q in range(1, PARTS):
            total = total + acc[q * rows:(q + 1) * rows, q * feats:(q + 1) * feats]
        return total * (1.0 / samples)

    def send_chunk(p, c):
        for d in others:
            rs_copy(p, d, c).start()
        on_helper(lambda: rs_copy(p, 0, c).start())

    def scatter(p, lhs):
        for c in range(len(chunks)):
            values = [(b, block_product(lhs, b)) for d in everyone for b in blocks_of(d, c)]
            for b, value in values:
                upd[p, b] = value
            send_chunk(p, c)

    def sum_and_gather(p, scale):
        def body():
            for c in range(len(chunks)):
                rs_arrivals(p, c).wait_recv()
                start, count = chunks[c]
                for k in range(start, start + count):
                    b = chip * per_owner + k
                    total = upd[p, b].astype(jnp.float32)
                    for slot in range(group - 1):
                        total = total + inbox[p, c, slot, k - start].astype(jnp.float32)
                    res[p, b] = res[p, b] - scale * total
                for d in others:
                    ag_copy(p, d, c).start()
                fw_copy(p, 0, c).start()
        on_owner(body)

    def gather_arrivals(p, use, early=False):
        for c in range(len(chunks)):
            if early and c == len(chunks) - 1:
                wait_scatter(p)
            def owning():
                for d in others[::-1]:
                    fw_copy(p, d, c).wait_recv()
                    fw_copy(p, d, c).start()

            def helper():
                for d in everyone[::-1]:
                    fw_copy(p, d, c).wait_recv()

            on_owner(owning)
            on_helper(helper)
            use([b for d in everyone for b in blocks_of(d, c)])

    def wait_scatter(p):
        for c in range(len(chunks)):
            for d in others:
                rs_copy(p, d, c).wait_send()

        def helper():
            for c in range(len(chunks)):
                rs_copy(p, 0, c).wait_send()

        on_helper(helper)

    def wait_gather(p):
        def owning():
            for c in range(len(chunks)):
                for d in others:
                    ag_copy(p, d, c).wait_send()
                for d in everyone:
                    fw_copy(p, d, c).wait_send()
        on_owner(owning)

    w_copy = pltpu.make_async_copy(w_hbm, w_in, w_sem)
    w_copy.start()
    for c in range(len(chunks)):
        for d in everyone:
            x_copy(d, c).start()
    on_owner(lambda: y_copy().start())

    barrier = pltpu.get_barrier_semaphore()
    for step in range(1, group):
        pl.semaphore_signal(barrier, inc=1, device_id={"feat": (me + step) % group}, device_id_type=MESH)
    w_copy.wait()
    start_weights = tuple(w_in[p * rows:(p + 1) * rows] for p in halves)
    start_lhs = jnp.concatenate([diagonal(start_weights[p]) for p in halves], axis=0)

    for c in range(len(chunks)):
        for d in everyone:
            x_copy(d, c).wait()
        for b in [b for d in everyone for b in blocks_of(d, c)]:
            both = lax.dot_general(start_lhs, jnp.concatenate(x_parts(b), axis=1), (((1,), (1,)), ((), ())),
                                   preferred_element_type=jnp.float32).astype(jnp.bfloat16)
            for p in halves:
                upd[p, b] = both[p * PARTS * rows:(p + 1) * PARTS * rows]
        if c == 0:
            pl.semaphore_wait(barrier, group - 1)
        send_chunk(0, c)
    for c in range(len(chunks)):
        send_chunk(1, c)

    def prepare(b, total):
        for q, part in enumerate(x_parts(b)):
            xt[b, q * feats:(q + 1) * feats] = part.T
            wide = part.astype(jnp.float32)
            total = total + jnp.sum((wide * wide).reshape(width // 8, 8, feats), axis=0)
        return total

    squares = jnp.zeros((8, feats), jnp.float32)
    squares = lax.fori_loop(0, blocks // 2, prepare, squares)

    def take_targets():
        y_copy().wait()
        for p in halves:
            for k in range(per_owner):
                res[p, chip * per_owner + k] = jnp.concatenate(
                    [y_in[p * rows:(p + 1) * rows, (k * PARTS + q) * width:(k * PARTS + q + 1) * width]
                     for q in range(PARTS)], axis=0)

    on_owner(take_targets)
    for p in halves:
        sum_and_gather(p, 1.0)
    squares = lax.fori_loop(blocks // 2, blocks, prepare, squares)
    step_size = samples / (group * jnp.sum(squares))

    def half_sweep(p, weights):
        acc = [jnp.zeros((PARTS * rows, PARTS * feats), jnp.float32)]

        def use(parts):
            for b in parts:
                acc[0] = acc[0] + gradient_term(res[p, b], b)

        gather_arrivals(p, use, True)
        coef = step_size * (gradient_of(acc[0]) - RIDGE * weights)
        for step_idx in range(1, LOCAL_STEPS):
            lhs = diagonal(coef)
            total = jnp.zeros((PARTS * rows, PARTS * feats), jnp.float32)
            queue = [block_product(lhs, b) for b in range(AHEAD)]
            for b in range(blocks):
                if b + AHEAD < blocks:
                    queue.append(block_product(lhs, b + AHEAD))
                product = queue.pop(0).astype(jnp.float32)
                total = total + gradient_term(res[p, b] - group * product, b)
            coef = coef + step_size * (gradient_of(total) - RIDGE * (weights + coef))
        wait_gather(p)
        scatter(p, diagonal(coef))
        return weights + GAMMA * coef

    def sweep(sweep_idx, weights):
        weights = tuple(half_sweep(p, weights[p]) for p in halves)
        for p in halves:
            sum_and_gather(p, GAMMA)
        return weights

    end_weights = lax.fori_loop(0, SWEEPS, sweep, start_weights)
    for p in halves:
        w_out[p * rows:(p + 1) * rows] = end_weights[p]

        def put(parts):
            for b in parts:
                for q in range(PARTS):
                    cols = pl.ds(pl.multiple_of((b * PARTS + q) * width, width), width)
                    r_out[p * rows:(p + 1) * rows, cols] = res[p, b, q * rows:(q + 1) * rows]

        gather_arrivals(p, put)
        wait_scatter(p)
        wait_gather(p)


def solution(mesh):
    group = mesh.shape["feat"]

    def per_device(design, w_init, targets):
        samples, feats = design.shape
        outs = targets.shape[1]
        chips = group // 2
        blocks = samples // (PARTS * LANES)
        per_owner = blocks // chips
        parts = len(CHUNKS)
        rows = PARTS * outs // 2
        hbm = pl.BlockSpec(memory_space=pltpu.HBM)
        vmem = pl.BlockSpec(memory_space=pltpu.VMEM)
        dma = pltpu.SemaphoreType.DMA
        weights, residual = pl.pallas_call(
            functools.partial(kernel, group, per_owner),
            out_shape=(jax.ShapeDtypeStruct((outs, feats), jnp.float32),
                       jax.ShapeDtypeStruct((outs, samples), jnp.float32)),
            in_specs=[hbm, hbm, hbm],
            out_specs=(vmem, vmem),
            scratch_shapes=[
                pltpu.VMEM((samples, feats), jnp.bfloat16),
                pltpu.VMEM((blocks, PARTS * feats, LANES), jnp.bfloat16),
                pltpu.VMEM((outs, feats), jnp.float32),
                dma,
                pltpu.VMEM((outs, per_owner * PARTS * LANES), jnp.float32),
                pltpu.VMEM((2, blocks, rows, LANES), jnp.float32),
                pltpu.VMEM((2, blocks, rows, LANES), jnp.bfloat16),
                pltpu.VMEM((2, parts, group - 1, per_owner // parts, rows, LANES), jnp.bfloat16),
                dma((chips, parts)),
                dma,
                dma((2, chips, parts)),
                dma((2, parts)),
                dma((2, chips, parts)),
                dma((2, chips, parts)),
                dma((2, chips, parts)),
            ],
            compiler_params=pltpu.CompilerParams(collective_id=0, has_side_effects=True,
                                                 vmem_limit_bytes=56000000),
        )(design, pltpu.with_memory_space_constraint(w_init.T, pltpu.HBM), targets.T)
        return weights.T, residual.T

    return jax.shard_map(
        per_device,
        mesh=mesh,
        in_specs=(P(None, ("prob", "feat")), P(("prob", "feat"), None), P("prob", None)),
        out_specs=(P(("prob", "feat"), None), P("prob", None)),
        check_vma=False,
    )
```

```python
import functools

import jax
import jax.numpy as jnp
from jax import lax
from jax.experimental import pallas as pl
from jax.experimental.pallas import tpu as pltpu
from jax.sharding import PartitionSpec as P

LOCAL_STEPS = 2
SWEEPS = 6
RIDGE = 0.01
GAMMA = 0.75

LANES = 256
PARTS = 4
CHUNKS = (2, 2)
AHEAD = 4
MESH = pl.DeviceIdType.MESH


def kernel(group, per_owner, x_hbm, w_hbm, y_hbm, w_out, r_out,
           x, xt, w_in, w_sem, y_in, res, upd, inbox,
           x_sem, y_sem, rs_send, rs_recv, ag_send, ag_recv, fw_send):
    chips = group // 2
    width = LANES
    blocks = chips * per_owner
    samples, feats = x.shape
    rows = w_in.shape[0] // 2
    size = PARTS * width
    halves = (0, 1)
    me = lax.axis_index("feat")
    chip, core = me // 2, me % 2

    others = sorted(range(1, chips), key=lambda d: -min(d, chips - d))
    everyone = others + [0]
    chunks = []
    for count in CHUNKS:
        chunks.append((sum(n for _, n in chunks), count))
    assert sum(CHUNKS) == per_owner

    def owner(d):
        return (chip + d) % chips

    def on_owner(body):
        pl.when(core == 1)(body)

    def on_helper(body):
        pl.when(core == 0)(body)

    def span(d, c):
        start, count = chunks[c]
        return pl.ds(owner(d) * per_owner + start, count)

    def blocks_of(d, c):
        start, count = chunks[c]
        return [owner(d) * per_owner + start + k for k in range(count)]

    def x_copy(d, c):
        start, count = chunks[c]
        part = pl.ds(pl.multiple_of((owner(d) * per_owner + start) * size, size), count * size)
        return pltpu.make_async_copy(x_hbm.at[part], x.at[part], x_sem.at[d, c])

    def y_copy():
        cols = pl.ds(pl.multiple_of(chip * (per_owner * size), per_owner * size), per_owner * size)
        return pltpu.make_async_copy(y_hbm.at[:, cols], y_in, y_sem)

    def remote(src, dst, send, recv, chip_to, core_to):
        return pltpu.make_async_remote_copy(src_ref=src, dst_ref=dst, send_sem=send, recv_sem=recv,
                                            device_id={"feat": chip_to * 2 + core_to}, device_id_type=MESH)

    def rs_copy(p, d, c):
        slot = ((chips - d) % chips * 2 + 1 - core + group - 1) % group
        start, count = chunks[c]
        return remote(upd.at[p, span(d, c)], inbox.at[p, c, slot],
                      rs_send.at[p, d, c], rs_recv.at[p, c], owner(d), 1)

    def rs_arrivals(p, c):
        return remote(inbox.at[p, c], inbox.at[p, c], rs_send.at[p, 0, c], rs_recv.at[p, c], chip, 0)

    def ag_copy(p, d, c):
        own = res.at[p, span(0, c)]
        return remote(own, own, ag_send.at[p, d, c], ag_recv.at[p, (chips - d) % chips, c], owner(d), 1)

    def fw_copy(p, d, c):
        part = res.at[p, span(d, c)]
        return remote(part, part, fw_send.at[p, d, c], ag_recv.at[p, d, c], chip, 0)

    def x_parts(b):
        start = pl.multiple_of(b * size, size)
        return [x[pl.ds(start + q * width, width)] for q in range(PARTS)]

    def diagonal(coef):
        tall = jnp.concatenate([coef] * PARTS, axis=0)
        place = lax.broadcasted_iota(jnp.int32, tall.shape, 0) // rows
        return jnp.concatenate([jnp.where(place == q, tall, 0.0) for q in range(PARTS)], axis=1).astype(jnp.bfloat16)

    def block_product(lhs, b):
        return jnp.dot(lhs, xt[b], preferred_element_type=jnp.float32).astype(jnp.bfloat16)

    def gradient_term(resid, b):
        return jnp.dot(resid.astype(jnp.bfloat16), jnp.concatenate(x_parts(b), axis=1),
                       preferred_element_type=jnp.float32)

    def gradient_of(acc):
        total = acc[:rows, :feats]
        for q in range(1, PARTS):
            total = total + acc[q * rows:(q + 1) * rows, q * feats:(q + 1) * feats]
        return total * (1.0 / samples)

    def send_chunk(p, c):
        for d in others:
            rs_copy(p, d, c).start()
        on_helper(lambda: rs_copy(p, 0, c).start())

    def scatter(p, lhs):
        last = len(chunks) - 1
        for c in range(len(chunks)):
            ds = others if c < last else everyone
            values = [(b, block_product(lhs, b)) for d in ds for b in blocks_of(d, c)]
            if c == last:
                values += [(b, block_product(lhs, b)) for k in range(last) for b in blocks_of(0, k)]
            for b, value in values:
                upd[p, b] = value
            for d in others:
                rs_copy(p, d, c).start()

        def to_owner():
            for c in range(len(chunks)):
                rs_copy(p, 0, c).start()

        on_helper(to_owner)

    def sum_and_gather(p, scale):
        def body():
            for c in range(len(chunks)):
                rs_arrivals(p, c).wait_recv()
                start, count = chunks[c]
                for k in range(start, start + count):
                    b = chip * per_owner + k
                    total = upd[p, b].astype(jnp.float32)
                    for slot in range(group - 1):
                        total = total + inbox[p, c, slot, k - start].astype(jnp.float32)
                    res[p, b] = res[p, b] - scale * total
                for d in others:
                    ag_copy(p, d, c).start()
                fw_copy(p, 0, c).start()
        on_owner(body)

    def gather_arrivals(p, use, early=False):
        for c in range(len(chunks)):
            if early and c == len(chunks) - 1:
                wait_scatter(p)
            def owning():
                for d in others[::-1]:
                    fw_copy(p, d, c).wait_recv()
                    fw_copy(p, d, c).start()

            def helper():
                for d in everyone[::-1]:
                    fw_copy(p, d, c).wait_recv()

            on_owner(owning)
            on_helper(helper)
            use([b for d in everyone for b in blocks_of(d, c)])

    def wait_scatter(p):
        for c in range(len(chunks)):
            for d in others:
                rs_copy(p, d, c).wait_send()

        def helper():
            for c in range(len(chunks)):
                rs_copy(p, 0, c).wait_send()

        on_helper(helper)

    def wait_gather(p):
        def owning():
            for c in range(len(chunks)):
                for d in others:
                    ag_copy(p, d, c).wait_send()
                for d in everyone:
                    fw_copy(p, d, c).wait_send()
        on_owner(owning)

    w_copy = pltpu.make_async_copy(w_hbm, w_in, w_sem)
    w_copy.start()
    for c in range(len(chunks)):
        for d in everyone:
            x_copy(d, c).start()
    on_owner(lambda: y_copy().start())

    barrier = pltpu.get_barrier_semaphore()
    for step in range(1, group):
        pl.semaphore_signal(barrier, inc=1, device_id={"feat": (me + step) % group}, device_id_type=MESH)
    w_copy.wait()
    start_weights = tuple(w_in[p * rows:(p + 1) * rows] for p in halves)
    start_lhs = jnp.concatenate([diagonal(start_weights[p]) for p in halves], axis=0)

    for c in range(len(chunks)):
        for d in everyone:
            x_copy(d, c).wait()
        for b in [b for d in everyone for b in blocks_of(d, c)]:
            both = lax.dot_general(start_lhs, jnp.concatenate(x_parts(b), axis=1), (((1,), (1,)), ((), ())),
                                   preferred_element_type=jnp.float32).astype(jnp.bfloat16)
            for p in halves:
                upd[p, b] = both[p * PARTS * rows:(p + 1) * PARTS * rows]
        if c == 0:
            pl.semaphore_wait(barrier, group - 1)
        send_chunk(0, c)
    for c in range(len(chunks)):
        send_chunk(1, c)

    def prepare(b, total):
        for q, part in enumerate(x_parts(b)):
            xt[b, q * feats:(q + 1) * feats] = part.T
            wide = part.astype(jnp.float32)
            total = total + jnp.sum((wide * wide).reshape(width // 8, 8, feats), axis=0)
        return total

    squares = jnp.zeros((8, feats), jnp.float32)
    squares = lax.fori_loop(0, blocks // 2, prepare, squares)

    def take_targets():
        y_copy().wait()
        for p in halves:
            for k in range(per_owner):
                res[p, chip * per_owner + k] = jnp.concatenate(
                    [y_in[p * rows:(p + 1) * rows, (k * PARTS + q) * width:(k * PARTS + q + 1) * width]
                     for q in range(PARTS)], axis=0)

    on_owner(take_targets)
    for p in halves:
        sum_and_gather(p, 1.0)
    squares = lax.fori_loop(blocks // 2, blocks, prepare, squares)
    step_size = samples / (group * jnp.sum(squares))

    def half_sweep(p, weights):
        acc = [jnp.zeros((PARTS * rows, PARTS * feats), jnp.float32)]

        def use(parts):
            for b in parts:
                acc[0] = acc[0] + gradient_term(res[p, b], b)

        gather_arrivals(p, use, True)
        coef = step_size * (gradient_of(acc[0]) - RIDGE * weights)
        for step_idx in range(1, LOCAL_STEPS):
            lhs = diagonal(coef)
            total = jnp.zeros((PARTS * rows, PARTS * feats), jnp.float32)
            queue = [block_product(lhs, b) for b in range(AHEAD)]
            for b in range(blocks):
                if b + AHEAD < blocks:
                    queue.append(block_product(lhs, b + AHEAD))
                product = queue.pop(0).astype(jnp.float32)
                total = total + gradient_term(res[p, b] - group * product, b)
            coef = coef + step_size * (gradient_of(total) - RIDGE * (weights + coef))
        wait_gather(p)
        scatter(p, diagonal(coef))
        return weights + GAMMA * coef

    def sweep(sweep_idx, weights):
        weights = tuple(half_sweep(p, weights[p]) for p in halves)
        for p in halves:
            sum_and_gather(p, GAMMA)
        return weights

    end_weights = lax.fori_loop(0, SWEEPS, sweep, start_weights)
    for p in halves:
        w_out[p * rows:(p + 1) * rows] = end_weights[p]

        def put(parts):
            for b in parts:
                for q in range(PARTS):
                    cols = pl.ds(pl.multiple_of((b * PARTS + q) * width, width), width)
                    r_out[p * rows:(p + 1) * rows, cols] = res[p, b, q * rows:(q + 1) * rows]

        gather_arrivals(p, put)
        wait_scatter(p)
        wait_gather(p)


def solution(mesh):
    group = mesh.shape["feat"]

    def per_device(design, w_init, targets):
        samples, feats = design.shape
        outs = targets.shape[1]
        chips = group // 2
        blocks = samples // (PARTS * LANES)
        per_owner = blocks // chips
        parts = len(CHUNKS)
        rows = PARTS * outs // 2
        hbm = pl.BlockSpec(memory_space=pltpu.HBM)
        vmem = pl.BlockSpec(memory_space=pltpu.VMEM)
        dma = pltpu.SemaphoreType.DMA
        weights, residual = pl.pallas_call(
            functools.partial(kernel, group, per_owner),
            out_shape=(jax.ShapeDtypeStruct((outs, feats), jnp.float32),
                       jax.ShapeDtypeStruct((outs, samples), jnp.float32)),
            in_specs=[hbm, hbm, hbm],
            out_specs=(vmem, vmem),
            scratch_shapes=[
                pltpu.VMEM((samples, feats), jnp.bfloat16),
                pltpu.VMEM((blocks, PARTS * feats, LANES), jnp.bfloat16),
                pltpu.VMEM((outs, feats), jnp.float32),
                dma,
                pltpu.VMEM((outs, per_owner * PARTS * LANES), jnp.float32),
                pltpu.VMEM((2, blocks, rows, LANES), jnp.float32),
                pltpu.VMEM((2, blocks, rows, LANES), jnp.bfloat16),
                pltpu.VMEM((2, parts, group - 1, per_owner // parts, rows, LANES), jnp.bfloat16),
                dma((chips, parts)),
                dma,
                dma((2, chips, parts)),
                dma((2, parts)),
                dma((2, chips, parts)),
                dma((2, chips, parts)),
                dma((2, chips, parts)),
            ],
            compiler_params=pltpu.CompilerParams(collective_id=0, has_side_effects=True,
                                                 vmem_limit_bytes=56000000),
        )(design, pltpu.with_memory_space_constraint(w_init.T, pltpu.HBM), targets.T)
        return weights.T, residual.T

    return jax.shard_map(
        per_device,
        mesh=mesh,
        in_specs=(P(None, ("prob", "feat")), P(("prob", "feat"), None), P("prob", None)),
        out_specs=(P(("prob", "feat"), None), P("prob", None)),
        check_vma=False,
    )
```

```python
import functools

import jax
import jax.numpy as jnp
from jax import lax
from jax.experimental import pallas as pl
from jax.experimental.pallas import tpu as pltpu
from jax.sharding import PartitionSpec as P

LOCAL_STEPS = 2
SWEEPS = 6
RIDGE = 0.01
GAMMA = 0.75

LANES = 256
PARTS = 4
CHUNKS = (2, 2)
AHEAD = 4
MESH = pl.DeviceIdType.MESH


def kernel(group, per_owner, x_hbm, w_hbm, y_hbm, w_out, r_out,
           x, xt, w_in, w_sem, y_in, res, upd, inbox,
           x_sem, y_sem, rs_send, rs_recv, ag_send, ag_recv, fw_send):
    chips = group // 2
    width = LANES
    blocks = chips * per_owner
    samples, feats = x.shape
    rows = w_in.shape[0] // 2
    size = PARTS * width
    halves = (0, 1)
    me = lax.axis_index("feat")
    chip, core = me // 2, me % 2

    others = sorted(range(1, chips), key=lambda d: -min(d, chips - d))
    everyone = others + [0]
    chunks = []
    for count in CHUNKS:
        chunks.append((sum(n for _, n in chunks), count))
    assert sum(CHUNKS) == per_owner

    def owner(d):
        return (chip + d) % chips

    def on_owner(body):
        pl.when(core == 1)(body)

    def on_helper(body):
        pl.when(core == 0)(body)

    def span(d, c):
        start, count = chunks[c]
        return pl.ds(owner(d) * per_owner + start, count)

    def blocks_of(d, c):
        start, count = chunks[c]
        return [owner(d) * per_owner + start + k for k in range(count)]

    def x_copy(d, c):
        start, count = chunks[c]
        part = pl.ds(pl.multiple_of((owner(d) * per_owner + start) * size, size), count * size)
        return pltpu.make_async_copy(x_hbm.at[part], x.at[part], x_sem.at[d, c])

    def y_copy():
        cols = pl.ds(pl.multiple_of(chip * (per_owner * size), per_owner * size), per_owner * size)
        return pltpu.make_async_copy(y_hbm.at[:, cols], y_in, y_sem)

    def remote(src, dst, send, recv, chip_to, core_to):
        return pltpu.make_async_remote_copy(src_ref=src, dst_ref=dst, send_sem=send, recv_sem=recv,
                                            device_id={"feat": chip_to * 2 + core_to}, device_id_type=MESH)

    def rs_copy(p, d, c):
        slot = ((chips - d) % chips * 2 + 1 - core + group - 1) % group
        start, count = chunks[c]
        return remote(upd.at[p, span(d, c)], inbox.at[p, c, slot],
                      rs_send.at[p, d, c], rs_recv.at[p, c], owner(d), 1)

    def rs_arrivals(p, c):
        return remote(inbox.at[p, c], inbox.at[p, c], rs_send.at[p, 0, c], rs_recv.at[p, c], chip, 0)

    def ag_copy(p, d, c):
        own = res.at[p, span(0, c)]
        return remote(own, own, ag_send.at[p, d, c], ag_recv.at[p, (chips - d) % chips, c], owner(d), 1)

    def fw_copy(p, d, c):
        part = res.at[p, span(d, c)]
        return remote(part, part, fw_send.at[p, d, c], ag_recv.at[p, d, c], chip, 0)

    def x_parts(b):
        start = pl.multiple_of(b * size, size)
        return [x[pl.ds(start + q * width, width)] for q in range(PARTS)]

    def diagonal(coef):
        tall = jnp.concatenate([coef] * PARTS, axis=0)
        place = lax.broadcasted_iota(jnp.int32, tall.shape, 0) // rows
        return jnp.concatenate([jnp.where(place == q, tall, 0.0) for q in range(PARTS)], axis=1).astype(jnp.bfloat16)

    def block_product(lhs, b):
        return jnp.dot(lhs, xt[b], preferred_element_type=jnp.float32).astype(jnp.bfloat16)

    def gradient_term(resid, b):
        return jnp.dot(resid.astype(jnp.bfloat16), jnp.concatenate(x_parts(b), axis=1),
                       preferred_element_type=jnp.float32)

    def gradient_of(acc):
        total = acc[:rows, :feats]
        for q in range(1, PARTS):
            total = total + acc[q * rows:(q + 1) * rows, q * feats:(q + 1) * feats]
        return total * (1.0 / samples)

    def send_chunk(p, c):
        for d in others:
            rs_copy(p, d, c).start()
        on_helper(lambda: rs_copy(p, 0, c).start())

    def scatter(p, lhs):
        last = len(chunks) - 1
        for c in range(len(chunks)):
            ds = others if c < last else everyone
            values = [(b, block_product(lhs, b)) for d in ds for b in blocks_of(d, c)]
            if c == last:
                values += [(b, block_product(lhs, b)) for k in range(last) for b in blocks_of(0, k)]
            for b, value in values:
                upd[p, b] = value
            for d in others:
                rs_copy(p, d, c).start()

        def to_owner():
            for c in range(len(chunks)):
                rs_copy(p, 0, c).start()

        on_helper(to_owner)

    def sum_and_gather(p, scale):
        def body():
            for c in range(len(chunks)):
                rs_arrivals(p, c).wait_recv()
                start, count = chunks[c]
                for k in range(start, start + count):
                    b = chip * per_owner + k
                    total = upd[p, b].astype(jnp.float32)
                    for slot in range(group - 1):
                        total = total + inbox[p, c, slot, k - start].astype(jnp.float32)
                    res[p, b] = res[p, b] - scale * total
                for d in others:
                    ag_copy(p, d, c).start()
                fw_copy(p, 0, c).start()
        on_owner(body)

    def gather_arrivals(p, use, early=False):
        for c in range(len(chunks)):
            if early and c == len(chunks) - 1:
                wait_scatter(p)
            def owning():
                for d in others[::-1]:
                    fw_copy(p, d, c).wait_recv()
                    fw_copy(p, d, c).start()

            def helper():
                for k in range(len(chunks) if c == 0 else 0):
                    fw_copy(p, 0, k).wait_recv()
                for d in others[::-1]:
                    fw_copy(p, d, c).wait_recv()

            on_owner(owning)
            on_helper(helper)
            own = [b for k in range(len(chunks)) for b in blocks_of(0, k)] if c == 0 else []
            use([b for d in others for b in blocks_of(d, c)] + own)

    def wait_scatter(p):
        for c in range(len(chunks)):
            for d in others:
                rs_copy(p, d, c).wait_send()

        def helper():
            for c in range(len(chunks)):
                rs_copy(p, 0, c).wait_send()

        on_helper(helper)

    def wait_gather(p):
        def owning():
            for c in range(len(chunks)):
                for d in others:
                    ag_copy(p, d, c).wait_send()
                for d in everyone:
                    fw_copy(p, d, c).wait_send()
        on_owner(owning)

    w_copy = pltpu.make_async_copy(w_hbm, w_in, w_sem)
    w_copy.start()
    for c in range(len(chunks)):
        for d in everyone:
            x_copy(d, c).start()
    on_owner(lambda: y_copy().start())

    barrier = pltpu.get_barrier_semaphore()
    for step in range(1, group):
        pl.semaphore_signal(barrier, inc=1, device_id={"feat": (me + step) % group}, device_id_type=MESH)
    w_copy.wait()
    start_weights = tuple(w_in[p * rows:(p + 1) * rows] for p in halves)
    start_lhs = jnp.concatenate([diagonal(start_weights[p]) for p in halves], axis=0)

    for c in range(len(chunks)):
        for d in everyone:
            x_copy(d, c).wait()
        for b in [b for d in everyone for b in blocks_of(d, c)]:
            both = lax.dot_general(start_lhs, jnp.concatenate(x_parts(b), axis=1), (((1,), (1,)), ((), ())),
                                   preferred_element_type=jnp.float32).astype(jnp.bfloat16)
            for p in halves:
                upd[p, b] = both[p * PARTS * rows:(p + 1) * PARTS * rows]
        if c == 0:
            pl.semaphore_wait(barrier, group - 1)
        send_chunk(0, c)
    for c in range(len(chunks)):
        send_chunk(1, c)

    def prepare(b, total):
        for q, part in enumerate(x_parts(b)):
            xt[b, q * feats:(q + 1) * feats] = part.T
            wide = part.astype(jnp.float32)
            total = total + jnp.sum((wide * wide).reshape(width // 8, 8, feats), axis=0)
        return total

    squares = jnp.zeros((8, feats), jnp.float32)
    squares = lax.fori_loop(0, blocks // 2, prepare, squares)

    def take_targets():
        y_copy().wait()
        for p in halves:
            for k in range(per_owner):
                res[p, chip * per_owner + k] = jnp.concatenate(
                    [y_in[p * rows:(p + 1) * rows, (k * PARTS + q) * width:(k * PARTS + q + 1) * width]
                     for q in range(PARTS)], axis=0)

    on_owner(take_targets)
    for p in halves:
        sum_and_gather(p, 1.0)
    squares = lax.fori_loop(blocks // 2, blocks, prepare, squares)
    step_size = samples / (group * jnp.sum(squares))

    def half_sweep(p, weights):
        acc = [jnp.zeros((PARTS * rows, PARTS * feats), jnp.float32)]

        def use(parts):
            for b in parts:
                acc[0] = acc[0] + gradient_term(res[p, b], b)

        gather_arrivals(p, use, True)
        coef = step_size * (gradient_of(acc[0]) - RIDGE * weights)
        for step_idx in range(1, LOCAL_STEPS):
            lhs = diagonal(coef)
            total = jnp.zeros((PARTS * rows, PARTS * feats), jnp.float32)
            queue = [block_product(lhs, b) for b in range(AHEAD)]
            for b in range(blocks):
                if b + AHEAD < blocks:
                    queue.append(block_product(lhs, b + AHEAD))
                product = queue.pop(0).astype(jnp.float32)
                total = total + gradient_term(res[p, b] - group * product, b)
            coef = coef + step_size * (gradient_of(total) - RIDGE * (weights + coef))
        wait_gather(p)
        scatter(p, diagonal(coef))
        return weights + GAMMA * coef

    def sweep(sweep_idx, weights):
        weights = tuple(half_sweep(p, weights[p]) for p in halves)
        for p in halves:
            sum_and_gather(p, GAMMA)
        return weights

    end_weights = lax.fori_loop(0, SWEEPS, sweep, start_weights)
    for p in halves:
        w_out[p * rows:(p + 1) * rows] = end_weights[p]

        def put(parts):
            for b in parts:
                for q in range(PARTS):
                    cols = pl.ds(pl.multiple_of((b * PARTS + q) * width, width), width)
                    r_out[p * rows:(p + 1) * rows, cols] = res[p, b, q * rows:(q + 1) * rows]

        gather_arrivals(p, put)
        wait_scatter(p)
        wait_gather(p)


def solution(mesh):
    group = mesh.shape["feat"]

    def per_device(design, w_init, targets):
        samples, feats = design.shape
        outs = targets.shape[1]
        chips = group // 2
        blocks = samples // (PARTS * LANES)
        per_owner = blocks // chips
        parts = len(CHUNKS)
        rows = PARTS * outs // 2
        hbm = pl.BlockSpec(memory_space=pltpu.HBM)
        vmem = pl.BlockSpec(memory_space=pltpu.VMEM)
        dma = pltpu.SemaphoreType.DMA
        weights, residual = pl.pallas_call(
            functools.partial(kernel, group, per_owner),
            out_shape=(jax.ShapeDtypeStruct((outs, feats), jnp.float32),
                       jax.ShapeDtypeStruct((outs, samples), jnp.float32)),
            in_specs=[hbm, hbm, hbm],
            out_specs=(vmem, vmem),
            scratch_shapes=[
                pltpu.VMEM((samples, feats), jnp.bfloat16),
                pltpu.VMEM((blocks, PARTS * feats, LANES), jnp.bfloat16),
                pltpu.VMEM((outs, feats), jnp.float32),
                dma,
                pltpu.VMEM((outs, per_owner * PARTS * LANES), jnp.float32),
                pltpu.VMEM((2, blocks, rows, LANES), jnp.float32),
                pltpu.VMEM((2, blocks, rows, LANES), jnp.bfloat16),
                pltpu.VMEM((2, parts, group - 1, per_owner // parts, rows, LANES), jnp.bfloat16),
                dma((chips, parts)),
                dma,
                dma((2, chips, parts)),
                dma((2, parts)),
                dma((2, chips, parts)),
                dma((2, chips, parts)),
                dma((2, chips, parts)),
            ],
            compiler_params=pltpu.CompilerParams(collective_id=0, has_side_effects=True,
                                                 vmem_limit_bytes=56000000),
        )(design, pltpu.with_memory_space_constraint(w_init.T, pltpu.HBM), targets.T)
        return weights.T, residual.T

    return jax.shard_map(
        per_device,
        mesh=mesh,
        in_specs=(P(None, ("prob", "feat")), P(("prob", "feat"), None), P("prob", None)),
        out_specs=(P(("prob", "feat"), None), P("prob", None)),
        check_vma=False,
    )
```
